32 devices in a mesh: row: 4 (over z), col: 4 (over y, core), rep: 2 (over x).
Axes of the slice: x: 2, y: 2, z: 4, core: 2. Of those that a mesh axis runs over, the one named last changes fastest.
Arguments:
- amplitudes: bfloat16 [1024, 8192], P('row', 'col'), may hold values from -6 to 6
- intermediate: bfloat16 [8192, 1024], P('row', 'col'), may hold values from -0.0625 to 0.0625
Outputs:
- residual: float32 [8, 4, 32, 1024], P(None, 'col', None, ('row', 'rep'))
The draws below stay inside these ranges and needn't reach their ends.
All inputs are finite; a program needn't handle non-finite values.
Results may differ from the reference program's by a relative error of at most 0.0029.
Values may be sent and summed in bfloat16 or wider, within the bound.
A program may use at most 128 MiB of HBM per device.

```python
import jax
import jax.numpy as jnp

KC_WIDTH = 8192
PAIR_DEV = 32
PAIRS = 1024
N_ROW = 4
N_COL = 4
N_REP = 2


def block_levels(rng, shape, cuts, least, largest):
    def one(dim, blocks):
        heights = jax.random.uniform(jax.random.fold_in(jax.random.fold_in(rng, 6), dim), (blocks,), jnp.float32, least / len(cuts), largest / len(cuts))
        return jnp.repeat(jnp.exp(heights), shape[dim] // blocks).reshape((-1,) + (1,) * (len(shape) - dim - 1))

    loudness = one(*cuts[0])
    for cut in cuts[1:]:
        loudness = loudness * one(*cut)
    return loudness


def scatter_about(stream_key, dims, width, bound, split=(), held_as=jnp.bfloat16):
    values = jax.random.normal(stream_key, dims, jnp.float32) * width
    if len(split) > 0:
        values = block_levels(stream_key, dims, split, -0.22, 0.18) * values
    return jnp.clip(values, min=-bound, max=bound).astype(held_as)


def setup_inputs(seed: int = 0) -> dict:
    keys = jax.random.split(jax.random.key(seed), 3)
    return {
        "amplitudes": scatter_about(keys[0], (PAIRS, KC_WIDTH), 1.0, 6.0, ((0, 4), (1, 4))),
        "intermediate": scatter_about(keys[1], (KC_WIDTH, PAIRS), KC_WIDTH ** -0.5, 0.0625, ((0, 4), (1, 4))),
    }


def reference(amplitudes, intermediate):
    cycle = jnp.dot(amplitudes, intermediate, preferred_element_type=jnp.float32).astype(jnp.bfloat16)
    widened = cycle.astype(jnp.float32)
    symmetric = widened + widened.T
    return symmetric.reshape(N_ROW * N_REP, N_COL, PAIR_DEV, PAIRS)
```

```python
import functools

import jax
import jax.numpy as jnp
from jax import lax
from jax.experimental import pallas as pl
from jax.experimental.pallas import tpu as pltpu
from jax.sharding import PartitionSpec as P

MESH = pl.DeviceIdType.MESH


def general(amplitudes, intermediate):
    rows_axis = lax.axis_size("row")
    cols_axis = lax.axis_size("col")
    depth_axis = lax.axis_size("rep")
    layer_index = lax.axis_index("rep")
    owner_rows = rows_axis * depth_axis
    fold_count = owner_rows // cols_axis
    local_rows = amplitudes.shape[0]
    band_rows = local_rows // depth_axis
    local_cols = intermediate.shape[1]
    slice_width = local_cols // owner_rows
    own_rows = lax.dynamic_slice_in_dim(amplitudes, layer_index * band_rows, band_rows, 0)
    all_weights = lax.all_gather(intermediate, "row", axis=0, tiled=True)
    summed = jnp.dot(
        lax.all_gather(own_rows, "col", axis=1, tiled=True),
        all_weights,
        preferred_element_type=jnp.float32,
    )
    cycle = summed.astype(jnp.bfloat16)
    spread_block = cycle.reshape(band_rows, fold_count, cols_axis, slice_width)
    direct = lax.all_to_all(spread_block, "col", split_axis=2, concat_axis=1, tiled=True).reshape(
        band_rows, owner_rows, slice_width
    )
    stacked = cycle.reshape(cols_axis, slice_width, fold_count, cols_axis * slice_width)
    mirror = lax.all_to_all(
        lax.all_to_all(stacked, "col", split_axis=0, concat_axis=2, tiled=True),
        ("row", "rep"),
        split_axis=2,
        concat_axis=0,
        tiled=True,
    )
    mirror_part = mirror.reshape(owner_rows, slice_width, band_rows).astype(jnp.float32)
    direct_part = jnp.transpose(direct, (1, 2, 0)).astype(jnp.float32)
    return (mirror_part + direct_part).reshape(owner_rows, 1, slice_width, band_rows)


def kernel(
    sizes, a_hbm, w_hbm, o_ref,
    a_v, w_v, relay, abuf, wbuf, p0, p1, r0, r1, cyc, spread, perm, drecv, mrecv,
    in_sem, s_rly, s_a, s_b, s_w1, s_w2, s_fw, s_r0, s_r1, s_m, s_d,
    q_rly, q_a, q_w1, q_w2, q_r0, q_r1, q_m, q_d,
):
    rows, cols, depth, chunks = sizes
    r, c, x = lax.axis_index("row"), lax.axis_index("col"), lax.axis_index("rep")
    y, u = c // 2, c % 2
    oy, ou, ox = 1 - y, 1 - u, 1 - x
    band, kc = a_v.shape
    width = w_v.shape[1]
    sub = band // (2 * depth)
    half = kc // 2
    slab = kc // (2 * chunks)
    strip = o_ref.shape[2]
    lanes = o_ref.shape[3]
    groups = width // (cols * strip)
    f32 = jnp.float32

    loads = (
        pltpu.make_async_copy(a_hbm, a_v, in_sem.at[0]),
        pltpu.make_async_copy(w_hbm, w_v, in_sem.at[1]),
    )
    for load in loads:
        load.start()

    barrier = pltpu.get_barrier_semaphore()
    total = rows * cols * depth
    me = (r * cols + c) * depth + x

    def greet(step, carry):
        other = (me + step) % total
        pl.semaphore_signal(
            barrier,
            inc=1,
            device_id=(other // (cols * depth), (other // depth) % cols, other % depth),
            device_id_type=MESH,
        )
        return carry

    lax.fori_loop(1, total, greet, 0)

    src = lax.broadcasted_iota(jnp.int32, (2 * width, 2 * width), 0)
    dst = lax.broadcasted_iota(jnp.int32, (2 * width, 2 * width), 1)
    lane_in = dst % strip
    grp = (dst // strip) % groups
    blk = (dst // (strip * groups)) % 2
    own = dst // (2 * strip * groups)
    perm[...] = jnp.where(
        src == blk * width + grp * (cols * strip) + own * strip + lane_in, 1.0, 0.0
    ).astype(jnp.bfloat16)

    pl.semaphore_wait(barrier, total - 1)
    loads[0].wait()

    def remote(source, target, send, recv, to):
        return pltpu.make_async_remote_copy(
            src_ref=source, dst_ref=target, send_sem=send, recv_sem=recv,
            device_id=to, device_id_type=MESH,
        )

    def arrived(target, recv):
        pltpu.make_async_copy(target, target, recv).wait()

    pending = []

    def send(source, target, ssem, rsem, to, same=None):
        copy = remote(source, target, ssem, rsem, to)
        if same is None:
            copy.start()
            pending.append((copy, None))
            return

        @pl.when(same)
        def _():
            pltpu.make_async_copy(source, target, rsem).start()

        @pl.when(jnp.logical_not(same))
        def _():
            copy.start()

        pending.append((copy, jnp.logical_not(same)))

    def rowset(side):
        return pl.ds(pl.multiple_of((x * 2 + side) * sub, sub), sub)

    def khalf(v):
        return pl.ds(v * half, half)

    for v in range(2):
        send(a_v.at[rowset(oy), khalf(v)], relay.at[:, khalf(v)], s_rly.at[v], q_rly.at[v], (r, oy * 2 + u, x))
    for v in range(2):
        send(
            a_v.at[rowset(y), khalf(v)], abuf.at[r, :, khalf(v)], s_a.at[v], q_a.at[r, v],
            (c, y * 2 + v, x), jnp.logical_and(c == r, u == v),
        )
    loads[1].wait()

    def wrows(side, n):
        return pl.ds(pl.multiple_of(side * half + n * slab, slab), slab)

    for n in range(chunks):
        send(w_v.at[wrows(x, n)], wbuf.at[wrows(x, n)], s_w1.at[n], q_w1.at[n], (r, oy * 2 + u, x))

    far = oy * 2 + u
    for v in range(2):
        arrived(relay.at[:, khalf(v)], q_rly.at[v])
        send(
            relay.at[:, khalf(v)], abuf.at[r, :, khalf(v)], s_b.at[v], q_a.at[r, v],
            (far, y * 2 + v, x), jnp.logical_and(far == r, u == v),
        )

    order = (r, r + 1 - 2 * (r % 2), (r + rows // 2) % rows, rows - 1 - r)

    def forward_w(n):
        arrived(wbuf.at[wrows(x, n)], q_w1.at[n])
        send(wbuf.at[wrows(x, n)], wbuf.at[wrows(x, n)], s_w2.at[n], q_w2.at[n], (r, c, ox))

    def forward_a(i):
        mine = pl.ds(pl.multiple_of(u * half, half), half)
        arrived(abuf.at[i, :, mine], q_a.at[i, u])
        send(abuf.at[i, :, mine], abuf.at[i, :, mine], s_fw.at[i], q_a.at[i, u], (r, y * 2 + ou, x))

    def product(i, d):
        theirs = pl.ds(pl.multiple_of(ou * half, half), half)
        arrived(abuf.at[i, :, theirs], q_a.at[i, ou])
        p0[i] = jnp.dot(abuf[i], w_v[...], preferred_element_type=f32)
        if d > 0:
            send(p0.at[i], r0.at[r], s_r0.at[i], q_r0.at[r], (i, c, x))

    steps = max(rows, chunks)
    for d in range(steps):
        if d < rows:
            forward_a(order[d])
        if d < chunks:
            forward_w(d)
        if 0 < d <= rows:
            product(order[d - 1], d - 1)
    if rows == steps:
        product(order[rows - 1], rows - 1)

    def add_product(side, n, first):
        at = pl.ds(pl.multiple_of(side * half + n * slab, slab), slab)
        part = jnp.dot(
            abuf[:, :, at].reshape(rows * sub, slab), wbuf[at, :], preferred_element_type=f32
        ).reshape(rows, sub, width)
        p1[...] = part if first else p1[...] + part

    for n in range(chunks):
        add_product(x, n, n == 0)
    for n in range(chunks):
        arrived(wbuf.at[wrows(ox, n)], q_w2.at[n])
        add_product(ox, n, False)
    for d in range(1, rows):
        i = order[d]
        send(p1.at[i], r1.at[r], s_r1.at[i], q_r1.at[r], (i, c, x))

    def finish(part, got, sems, q, block):
        value = part[r]
        for d in range(1, rows):
            i = order[d]
            arrived(got.at[i], sems.at[i])
            value = value + got[i]
        cyc[block] = value.astype(jnp.bfloat16)
        owner = block * 2 + u
        for px in range(depth):
            for pu in range(2):
                same = jnp.logical_and(jnp.logical_and(owner == r, px == x), pu == u)
                send(
                    cyc.at[block, pl.ds(pu * strip, strip), pl.ds(px * lanes, lanes)],
                    mrecv.at[r * depth + x],
                    s_m.at[q, px, pu], q_m.at[r * depth + x], (owner, y * 2 + pu, px), same,
                )

    finish(p0, r0, q_r0, 0, y)
    finish(p1, r1, q_r1, 1, oy)

    turned = jnp.dot(cyc[0], perm[pl.ds(0, width), :], preferred_element_type=f32)
    turned = turned + jnp.dot(cyc[1], perm[pl.ds(width, width), :], preferred_element_type=f32)
    for to in range(cols):
        spread[to] = turned[:, to * lanes:(to + 1) * lanes].astype(jnp.bfloat16)
    place = pl.ds(pl.multiple_of(y * sub, sub), sub)
    for to in range(cols):
        send(spread.at[to], drecv.at[u, place, :], s_d.at[to], q_d.at[u, y], (r, to, x), c == to)

    for i in range(rows * depth):
        arrived(mrecv.at[i], q_m.at[i])
    for pu in range(2):
        for py in range(2):
            arrived(drecv.at[pu, pl.ds(py * sub, sub), :], q_d.at[pu, py])
        flipped = jnp.transpose(drecv[pu].astype(f32))
        for py in range(2):
            for g in range(groups):
                at = (py * groups + g) * strip
                a = (py * 2 + pu) * groups + g
                o_ref[a, 0] = mrecv[a].astype(f32) + flipped[at:at + strip, :]

    for copy, sent in pending:
        if sent is None:
            copy.wait_send()
        else:
            pl.when(sent)(copy.wait_send)


def planned(sizes, amplitudes, intermediate):
    rows, cols, depth, chunks = sizes
    band, kc = amplitudes.shape
    width = intermediate.shape[1]
    sub = band // (2 * depth)
    owners = rows * depth
    strip = width // owners
    lanes = band // depth
    bf16, f32 = jnp.bfloat16, jnp.float32
    dma = pltpu.SemaphoreType.DMA
    return pl.pallas_call(
        functools.partial(kernel, sizes),
        out_shape=jax.ShapeDtypeStruct((owners, 1, strip, lanes), f32),
        in_specs=[pl.BlockSpec(memory_space=pl.ANY)] * 2,
        out_specs=pl.BlockSpec(memory_space=pltpu.VMEM),
        scratch_shapes=[
            pltpu.VMEM((band, kc), bf16),
            pltpu.VMEM((kc, width), bf16),
            pltpu.VMEM((sub, kc), bf16),
            pltpu.VMEM((rows, sub, kc), bf16),
            pltpu.VMEM((kc, width), bf16),
            pltpu.VMEM((rows, sub, width), f32),
            pltpu.VMEM((rows, sub, width), f32),
            pltpu.VMEM((rows, sub, width), f32),
            pltpu.VMEM((rows, sub, width), f32),
            pltpu.VMEM((2, sub, width), bf16),
            pltpu.VMEM((cols, sub, lanes), bf16),
            pltpu.VMEM((2 * width, 2 * width), bf16),
            pltpu.VMEM((2, 2 * sub, lanes), bf16),
            pltpu.VMEM((owners, strip, lanes), bf16),
            dma((2,)), dma((2,)), dma((2,)), dma((2,)), dma((chunks,)), dma((chunks,)),
            dma((rows,)), dma((rows,)), dma((rows,)), dma((2, depth, 2)), dma((cols,)),
            dma((2,)), dma((rows, 2)), dma((chunks,)), dma((chunks,)),
            dma((rows,)), dma((rows,)), dma((owners,)), dma((2, 2)),
        ],
        compiler_params=pltpu.CompilerParams(collective_id=0, has_side_effects=True),
    )(amplitudes, intermediate)


def solution(mesh):
    rows, cols, depth = (mesh.shape[name] for name in ("row", "col", "rep"))

    def local(amplitudes, intermediate):
        square = rows == cols == 2 * depth and depth == 2
        fits = amplitudes.shape[0] == intermediate.shape[1]
        if square and fits:
            return planned((rows, cols, depth, 4), amplitudes, intermediate)
        return general(amplitudes, intermediate)

    in_specs = (P("row", "col"), P("row", "col"))
    out_specs = P(None, "col", None, ("row", "rep"))
    return jax.shard_map(local, mesh=mesh, in_specs=in_specs, out_specs=out_specs, check_vma=False)
```

```python
import functools

import jax
import jax.numpy as jnp
from jax import lax
from jax.experimental import pallas as pl
from jax.experimental.pallas import tpu as pltpu
from jax.sharding import PartitionSpec as P

MESH = pl.DeviceIdType.MESH


def general(amplitudes, intermediate):
    rows_axis = lax.axis_size("row")
    cols_axis = lax.axis_size("col")
    depth_axis = lax.axis_size("rep")
    layer_index = lax.axis_index("rep")
    owner_rows = rows_axis * depth_axis
    fold_count = owner_rows // cols_axis
    local_rows = amplitudes.shape[0]
    band_rows = local_rows // depth_axis
    local_cols = intermediate.shape[1]
    slice_width = local_cols // owner_rows
    own_rows = lax.dynamic_slice_in_dim(amplitudes, layer_index * band_rows, band_rows, 0)
    all_weights = lax.all_gather(intermediate, "row", axis=0, tiled=True)
    summed = jnp.dot(
        lax.all_gather(own_rows, "col", axis=1, tiled=True),
        all_weights,
        preferred_element_type=jnp.float32,
    )
    cycle = summed.astype(jnp.bfloat16)
    spread_block = cycle.reshape(band_rows, fold_count, cols_axis, slice_width)
    direct = lax.all_to_all(spread_block, "col", split_axis=2, concat_axis=1, tiled=True).reshape(
        band_rows, owner_rows, slice_width
    )
    stacked = cycle.reshape(cols_axis, slice_width, fold_count, cols_axis * slice_width)
    mirror = lax.all_to_all(
        lax.all_to_all(stacked, "col", split_axis=0, concat_axis=2, tiled=True),
        ("row", "rep"),
        split_axis=2,
        concat_axis=0,
        tiled=True,
    )
    mirror_part = mirror.reshape(owner_rows, slice_width, band_rows).astype(jnp.float32)
    direct_part = jnp.transpose(direct, (1, 2, 0)).astype(jnp.float32)
    return (mirror_part + direct_part).reshape(owner_rows, 1, slice_width, band_rows)


def kernel(
    sizes, a_hbm, w_hbm, o_ref,
    a_v, w_v, relay, abuf, wbuf, p0, p1, r0, r1, turn, cyc, spread, perm, drecv, mrecv,
    in_sem, s_rly, s_a, s_b, s_w1, s_w2, s_fw, s_r0, s_r1, s_m, s_d,
    q_rly, q_a, q_w1, q_w2, q_r0, q_r1, q_m, q_d,
):
    rows, cols, depth, chunks = sizes
    r, c, x = lax.axis_index("row"), lax.axis_index("col"), lax.axis_index("rep")
    y, u = c // 2, c % 2
    oy, ou, ox = 1 - y, 1 - u, 1 - x
    sub, kc = a_v.shape[1:]
    width = w_v.shape[1]
    half = kc // 2
    slab = half // chunks
    strip = o_ref.shape[2]
    lanes = o_ref.shape[3]
    groups = width // (cols * strip)
    f32 = jnp.float32

    def rowset(side):
        return pl.ds(pl.multiple_of((x * 2 + side) * sub, sub), sub)

    def khalf(v):
        return pl.ds(v * half, half)

    def side_rows(side):
        return pl.ds(pl.multiple_of(side * half, half), half)

    loads = (
        pltpu.make_async_copy(a_hbm.at[rowset(oy)], a_v.at[0], in_sem.at[0]),
        pltpu.make_async_copy(a_hbm.at[rowset(y)], a_v.at[1], in_sem.at[1]),
        pltpu.make_async_copy(w_hbm.at[side_rows(x)], w_v.at[side_rows(x)], in_sem.at[2]),
        pltpu.make_async_copy(w_hbm.at[side_rows(ox)], w_v.at[side_rows(ox)], in_sem.at[3]),
    )
    for load in loads:
        load.start()

    barrier = pltpu.get_barrier_semaphore()
    total = rows * cols * depth
    me = (r * cols + c) * depth + x

    def greet(step, carry):
        other = (me + step) % total
        pl.semaphore_signal(
            barrier,
            inc=1,
            device_id=(other // (cols * depth), (other // depth) % cols, other % depth),
            device_id_type=MESH,
        )
        return carry

    lax.fori_loop(1, total, greet, 0)

    pl.semaphore_wait(barrier, total - 1)
    loads[0].wait()

    def remote(source, target, send, recv, to):
        return pltpu.make_async_remote_copy(
            src_ref=source, dst_ref=target, send_sem=send, recv_sem=recv,
            device_id=to, device_id_type=MESH,
        )

    def arrived(target, recv):
        pltpu.make_async_copy(target, target, recv).wait()

    pending = []

    def send(source, target, ssem, rsem, to, same=None):
        copy = remote(source, target, ssem, rsem, to)
        if same is None:
            copy.start()
            pending.append((copy, None))
            return

        @pl.when(same)
        def _():
            pltpu.make_async_copy(source, target, rsem).start()

        @pl.when(jnp.logical_not(same))
        def _():
            copy.start()

        pending.append((copy, jnp.logical_not(same)))

    rises = [(v, t) for v in range(2) for t in range(2)]

    def piece(v, t):
        return pl.ds(t * (sub // 2), sub // 2), khalf(v)

    for v, t in rises:
        at, ks = piece(v, t)
        send(
            a_v.at[0, at, ks], relay.at[at, ks], s_rly.at[v, t], q_rly.at[v, t],
            (r, oy * 2 + u, x),
        )
    loads[1].wait()
    for v in range(2):
        send(
            a_v.at[1, :, khalf(v)], abuf.at[r, :, khalf(v)], s_a.at[v], q_a.at[r, v],
            (c, y * 2 + v, x), jnp.logical_and(c == r, u == v),
        )
    loads[2].wait()

    def krows(side, n):
        return pl.ds(pl.multiple_of(side * half + n * slab, slab), slab)

    def wpart(ref, side, n, h):
        return ref.at[krows(side, n), pl.ds(h * lanes, lanes)]

    for h in range(depth):
        for n in range(chunks):
            send(
                wpart(w_v, x, n, h), wpart(wbuf, x, n, h), s_w1.at[h, n], q_w1.at[h, n],
                (r, oy * 2 + u, x),
            )

    far = oy * 2 + u
    for v, t in rises:
        at, ks = piece(v, t)
        arrived(relay.at[at, ks], q_rly.at[v, t])
        send(
            relay.at[at, ks], abuf.at[r, at, ks], s_b.at[v, t], q_a.at[r, v],
            (far, y * 2 + v, x), jnp.logical_and(far == r, u == v),
        )
    loads[3].wait()

    src = lax.broadcasted_iota(jnp.int32, (2 * width, 2 * width), 0)
    dst = lax.broadcasted_iota(jnp.int32, (2 * width, 2 * width), 1)
    lane_in = dst % strip
    grp = (dst // strip) % groups
    blk = (dst // (strip * groups)) % 2
    own = dst // (2 * strip * groups)
    perm[...] = jnp.where(
        src == blk * width + grp * (cols * strip) + own * strip + lane_in, 1.0, 0.0
    ).astype(jnp.bfloat16)

    order = (r, r + 1 - 2 * (r % 2), (r + rows // 2) % rows, rows - 1 - r)

    def forward_w(h, n):
        arrived(wpart(wbuf, x, n, h), q_w1.at[h, n])
        send(
            wpart(wbuf, x, n, h), wpart(wbuf, x, n, h), s_w2.at[h, n], q_w2.at[h, n], (r, c, ox)
        )

    def forward_a(i):
        mine = side_rows(u)
        arrived(abuf.at[i, :, mine], q_a.at[i, u])
        send(abuf.at[i, :, mine], abuf.at[i, :, mine], s_fw.at[i], q_a.at[i, u], (r, y * 2 + ou, x))

    def product(d):
        i = order[d]
        arrived(abuf.at[i, :, side_rows(ou)], q_a.at[i, ou])
        p0[i] = jnp.dot(abuf[i], w_v[...], preferred_element_type=f32)
        if d > 0:
            send(p0.at[i], r0.at[r], s_r0.at[i], q_r0.at[r], (i, c, x))

    hops = [(h, n) for h in range(depth) for n in range(chunks)]
    each = len(hops) // rows
    for d in range(rows):
        forward_a(order[d])
        product(d)
        for h, n in hops[d * each:(d + 1) * each]:
            forward_w(h, n)

    def add_product(side, n, h, first):
        part = jnp.dot(
            abuf[:, :, krows(side, n)].reshape(rows * sub, slab),
            wbuf[krows(side, n), pl.ds(h * lanes, lanes)],
            preferred_element_type=f32,
        ).reshape(rows, sub, lanes)
        p1[h] = part if first else p1[h] + part

    def other_product(h):
        for n in range(chunks):
            add_product(x, n, h, n == 0)
        for n in range(chunks):
            arrived(wpart(wbuf, ox, n, h), q_w2.at[h, n])
            add_product(ox, n, h, False)
        for d in range(1, rows):
            i = order[d]
            send(p1.at[h, i], r1.at[h, r], s_r1.at[h, i], q_r1.at[h, r], (i, c, x))

    def mirror(q, block, px):
        owner = block * 2 + u
        for pu in range(2):
            same = jnp.logical_and(jnp.logical_and(owner == r, px == x), pu == u)
            send(
                cyc.at[block, pl.ds(pu * strip, strip), pl.ds(px * lanes, lanes)],
                mrecv.at[r * depth + x],
                s_m.at[q, px, pu], q_m.at[r * depth + x], (owner, y * 2 + pu, px), same,
            )

    def finish_own():
        value = p0[r]
        for d in range(1, rows):
            i = order[d]
            arrived(r0.at[i], q_r0.at[i])
            value = value + r0[i]
        value = value.astype(jnp.bfloat16)
        cyc[y] = value
        for px in range(depth):
            mirror(0, y, px)
        rows_of = pl.ds(pl.multiple_of(y * width, width), width)
        turn[...] = jnp.dot(value, perm[rows_of, :], preferred_element_type=f32)

    def finish_other(h):
        value = p1[h, r]
        for d in range(1, rows):
            i = order[d]
            arrived(r1.at[h, i], q_r1.at[h, i])
            value = value + r1[h, i]
        value = value.astype(jnp.bfloat16)
        cyc[oy, :, pl.ds(h * lanes, lanes)] = value
        mirror(1, oy, h)
        rows_of = pl.ds(pl.multiple_of(oy * width + h * lanes, lanes), lanes)
        return turn[...] + jnp.dot(value, perm[rows_of, :], preferred_element_type=f32)

    other_product(0)
    finish_own()
    for h in range(1, depth):
        other_product(h)
        turn[...] = finish_other(h - 1)
    turned = finish_other(depth - 1)

    for to in range(cols):
        spread[to] = turned[:, to * lanes:(to + 1) * lanes].astype(jnp.bfloat16)
    place = pl.ds(pl.multiple_of(y * sub, sub), sub)
    for to in range(cols):
        send(spread.at[to], drecv.at[u, place, :], s_d.at[to], q_d.at[u, y], (r, to, x), c == to)

    for i in range(rows * depth):
        arrived(mrecv.at[i], q_m.at[i])
    for pu in range(2):
        for py in range(2):
            arrived(drecv.at[pu, pl.ds(py * sub, sub), :], q_d.at[pu, py])
        flipped = jnp.transpose(drecv[pu].astype(f32))
        for py in range(2):
            for g in range(groups):
                at = (py * groups + g) * strip
                a = (py * 2 + pu) * groups + g
                o_ref[a, 0] = mrecv[a].astype(f32) + flipped[at:at + strip, :]

    for copy, sent in pending:
        if sent is None:
            copy.wait_send()
        else:
            pl.when(sent)(copy.wait_send)


def planned(sizes, amplitudes, intermediate):
    rows, cols, depth, chunks = sizes
    band, kc = amplitudes.shape
    width = intermediate.shape[1]
    sub = band // (2 * depth)
    owners = rows * depth
    strip = width // owners
    lanes = band // depth
    bf16, f32 = jnp.bfloat16, jnp.float32
    dma = pltpu.SemaphoreType.DMA
    return pl.pallas_call(
        functools.partial(kernel, sizes),
        out_shape=jax.ShapeDtypeStruct((owners, 1, strip, lanes), f32),
        in_specs=[pl.BlockSpec(memory_space=pl.ANY)] * 2,
        out_specs=pl.BlockSpec(memory_space=pltpu.VMEM),
        scratch_shapes=[
            pltpu.VMEM((2, sub, kc), bf16),
            pltpu.VMEM((kc, width), bf16),
            pltpu.VMEM((sub, kc), bf16),
            pltpu.VMEM((rows, sub, kc), bf16),
            pltpu.VMEM((kc, width), bf16),
            pltpu.VMEM((rows, sub, width), f32),
            pltpu.VMEM((depth, rows, sub, lanes), f32),
            pltpu.VMEM((rows, sub, width), f32),
            pltpu.VMEM((depth, rows, sub, lanes), f32),
            pltpu.VMEM((sub, 2 * width), f32),
            pltpu.VMEM((2, sub, width), bf16),
            pltpu.VMEM((cols, sub, lanes), bf16),
            pltpu.VMEM((2 * width, 2 * width), bf16),
            pltpu.VMEM((2, 2 * sub, lanes), bf16),
            pltpu.VMEM((owners, strip, lanes), bf16),
            dma((4,)), dma((2, 2)), dma((2,)), dma((2, 2)), dma((depth, chunks)), dma((depth, chunks)),
            dma((rows,)), dma((rows,)), dma((depth, rows)), dma((2, depth, 2)), dma((cols,)),
            dma((2, 2)), dma((rows, 2)), dma((depth, chunks)), dma((depth, chunks)),
            dma((rows,)), dma((depth, rows)), dma((owners,)), dma((2, 2)),
        ],
        compiler_params=pltpu.CompilerParams(collective_id=0, has_side_effects=True),
    )(amplitudes, intermediate)


def solution(mesh):
    rows, cols, depth = (mesh.shape[name] for name in ("row", "col", "rep"))

    def local(amplitudes, intermediate):
        square = rows == cols == 2 * depth and depth == 2
        fits = amplitudes.shape[0] == intermediate.shape[1]
        if square and fits:
            return planned((rows, cols, depth, 4), amplitudes, intermediate)
        return general(amplitudes, intermediate)

    in_specs = (P("row", "col"), P("row", "col"))
    out_specs = P(None, "col", None, ("row", "rep"))
    return jax.shard_map(local, mesh=mesh, in_specs=in_specs, out_specs=out_specs, check_vma=False)
```

```python
import functools

import jax
import jax.numpy as jnp
from jax import lax
from jax.experimental import pallas as pl
from jax.experimental.pallas import tpu as pltpu
from jax.sharding import PartitionSpec as P

MESH = pl.DeviceIdType.MESH


def general(amplitudes, intermediate):
    rows_axis = lax.axis_size("row")
    cols_axis = lax.axis_size("col")
    depth_axis = lax.axis_size("rep")
    layer_index = lax.axis_index("rep")
    owner_rows = rows_axis * depth_axis
    fold_count = owner_rows // cols_axis
    local_rows = amplitudes.shape[0]
    band_rows = local_rows // depth_axis
    local_cols = intermediate.shape[1]
    slice_width = local_cols // owner_rows
    own_rows = lax.dynamic_slice_in_dim(amplitudes, layer_index * band_rows, band_rows, 0)
    all_weights = lax.all_gather(intermediate, "row", axis=0, tiled=True)
    summed = jnp.dot(
        lax.all_gather(own_rows, "col", axis=1, tiled=True),
        all_weights,
        preferred_element_type=jnp.float32,
    )
    cycle = summed.astype(jnp.bfloat16)
    spread_block = cycle.reshape(band_rows, fold_count, cols_axis, slice_width)
    direct = lax.all_to_all(spread_block, "col", split_axis=2, concat_axis=1, tiled=True).reshape(
        band_rows, owner_rows, slice_width
    )
    stacked = cycle.reshape(cols_axis, slice_width, fold_count, cols_axis * slice_width)
    mirror = lax.all_to_all(
        lax.all_to_all(stacked, "col", split_axis=0, concat_axis=2, tiled=True),
        ("row", "rep"),
        split_axis=2,
        concat_axis=0,
        tiled=True,
    )
    mirror_part = mirror.reshape(owner_rows, slice_width, band_rows).astype(jnp.float32)
    direct_part = jnp.transpose(direct, (1, 2, 0)).astype(jnp.float32)
    return (mirror_part + direct_part).reshape(owner_rows, 1, slice_width, band_rows)


def kernel(
    sizes, a_hbm, w_hbm, o_ref,
    a_v, w_v, relay, abuf, wbuf, p0, p1, r0, r1, turn, cyc, spread, perm, drecv, mrecv,
    in_sem, s_rly, s_a, s_b, s_w1, s_w2, s_fw, s_r0, s_r1, s_m, s_d,
    q_rly, q_a, q_w1, q_w2, q_r0, q_r1, q_m, q_d,
):
    rows, cols, depth, chunks = sizes
    r, c, x = lax.axis_index("row"), lax.axis_index("col"), lax.axis_index("rep")
    y, u = c // 2, c % 2
    oy, ou, ox = 1 - y, 1 - u, 1 - x
    sub, kc = a_v.shape[1:]
    width = w_v.shape[1]
    half = kc // 2
    slab = half // chunks
    strip = o_ref.shape[2]
    lanes = o_ref.shape[3]
    groups = width // (cols * strip)
    f32 = jnp.float32

    def rowset(side):
        return pl.ds(pl.multiple_of((x * 2 + side) * sub, sub), sub)

    def khalf(v):
        return pl.ds(v * half, half)

    def side_rows(side):
        return pl.ds(pl.multiple_of(side * half, half), half)

    loads = (
        pltpu.make_async_copy(a_hbm.at[rowset(oy)], a_v.at[0], in_sem.at[0]),
        pltpu.make_async_copy(a_hbm.at[rowset(y)], a_v.at[1], in_sem.at[1]),
        pltpu.make_async_copy(w_hbm.at[side_rows(x)], w_v.at[side_rows(x)], in_sem.at[2]),
        pltpu.make_async_copy(w_hbm.at[side_rows(ox)], w_v.at[side_rows(ox)], in_sem.at[3]),
    )
    for load in loads:
        load.start()

    barrier = pltpu.get_barrier_semaphore()
    total = rows * cols * depth
    me = (r * cols + c) * depth + x

    def greet(step, carry):
        other = (me + step) % total
        pl.semaphore_signal(
            barrier,
            inc=1,
            device_id=(other // (cols * depth), (other // depth) % cols, other % depth),
            device_id_type=MESH,
        )
        return carry

    lax.fori_loop(1, total, greet, 0)

    pl.semaphore_wait(barrier, total - 1)
    loads[0].wait()

    def remote(source, target, send, recv, to):
        return pltpu.make_async_remote_copy(
            src_ref=source, dst_ref=target, send_sem=send, recv_sem=recv,
            device_id=to, device_id_type=MESH,
        )

    def arrived(target, recv):
        pltpu.make_async_copy(target, target, recv).wait()

    pending = []

    def send(source, target, ssem, rsem, to, same=None):
        copy = remote(source, target, ssem, rsem, to)
        if same is None:
            copy.start()
            pending.append((copy, None))
            return

        @pl.when(same)
        def _():
            pltpu.make_async_copy(source, target, rsem).start()

        @pl.when(jnp.logical_not(same))
        def _():
            copy.start()

        pending.append((copy, jnp.logical_not(same)))

    rises = [(v, t) for v in range(2) for t in range(4)]

    def piece(v, t):
        return pl.ds(t * (sub // 4), sub // 4), khalf(v)

    for v, t in rises:
        at, ks = piece(v, t)
        send(
            a_v.at[0, at, ks], relay.at[at, ks], s_rly.at[v, t], q_rly.at[v, t],
            (r, oy * 2 + u, x),
        )
    loads[1].wait()
    for v in range(2):
        send(
            a_v.at[1, :, khalf(v)], abuf.at[r, :, khalf(v)], s_a.at[v], q_a.at[r, v],
            (c, y * 2 + v, x), jnp.logical_and(c == r, u == v),
        )
    loads[2].wait()

    def krows(side, n):
        return pl.ds(pl.multiple_of(side * half + n * slab, slab), slab)

    def wpart(ref, side, n, h):
        return ref.at[krows(side, n), pl.ds(h * lanes, lanes)]

    for h in range(depth):
        for n in range(chunks):
            send(
                wpart(w_v, x, n, h), wpart(wbuf, x, n, h), s_w1.at[h, n], q_w1.at[h, n],
                (r, oy * 2 + u, x),
            )

    far = oy * 2 + u
    for v, t in rises:
        at, ks = piece(v, t)
        arrived(relay.at[at, ks], q_rly.at[v, t])
        send(
            relay.at[at, ks], abuf.at[r, at, ks], s_b.at[v, t], q_a.at[r, v],
            (far, y * 2 + v, x), jnp.logical_and(far == r, u == v),
        )
    loads[3].wait()

    src = lax.broadcasted_iota(jnp.int32, (2 * width, 2 * width), 0)
    dst = lax.broadcasted_iota(jnp.int32, (2 * width, 2 * width), 1)
    lane_in = dst % strip
    grp = (dst // strip) % groups
    blk = (dst // (strip * groups)) % 2
    own = dst // (2 * strip * groups)
    perm[...] = jnp.where(
        src == blk * width + grp * (cols * strip) + own * strip + lane_in, 1.0, 0.0
    ).astype(jnp.bfloat16)

    order = (r, r + 1 - 2 * (r % 2), (r + rows // 2) % rows, rows - 1 - r)

    def forward_w(h, n):
        arrived(wpart(wbuf, x, n, h), q_w1.at[h, n])
        send(
            wpart(wbuf, x, n, h), wpart(wbuf, x, n, h), s_w2.at[h, n], q_w2.at[h, n], (r, c, ox)
        )

    def forward_a(i):
        mine = side_rows(u)
        arrived(abuf.at[i, :, mine], q_a.at[i, u])
        send(abuf.at[i, :, mine], abuf.at[i, :, mine], s_fw.at[i], q_a.at[i, u], (r, y * 2 + ou, x))

    def product(d):
        i = order[d]
        arrived(abuf.at[i, :, side_rows(ou)], q_a.at[i, ou])
        p0[i] = jnp.dot(abuf[i], w_v[...], preferred_element_type=f32)
        if d > 0:
            send(p0.at[i], r0.at[r], s_r0.at[i], q_r0.at[r], (i, c, x))

    hops = [(h, n) for h in range(depth) for n in range(chunks)]
    each = len(hops) // rows
    for d in range(rows):
        forward_a(order[d])
        product(d)
        for h, n in hops[d * each:(d + 1) * each]:
            forward_w(h, n)

    def add_product(side, n, h, first):
        part = jnp.dot(
            abuf[:, :, krows(side, n)].reshape(rows * sub, slab),
            wbuf[krows(side, n), pl.ds(h * lanes, lanes)],
            preferred_element_type=f32,
        ).reshape(rows, sub, lanes)
        p1[h] = part if first else p1[h] + part

    def other_product(h):
        for n in range(chunks):
            add_product(x, n, h, n == 0)
        for n in range(chunks):
            arrived(wpart(wbuf, ox, n, h), q_w2.at[h, n])
            add_product(ox, n, h, False)
        for d in range(1, rows):
            i = order[d]
            send(p1.at[h, i], r1.at[h, r], s_r1.at[h, i], q_r1.at[h, r], (i, c, x))

    def mirror(q, block, px):
        owner = block * 2 + u
        for pu in range(2):
            same = jnp.logical_and(jnp.logical_and(owner == r, px == x), pu == u)
            send(
                cyc.at[block, pl.ds(pu * strip, strip), pl.ds(px * lanes, lanes)],
                mrecv.at[r * depth + x],
                s_m.at[q, px, pu], q_m.at[r * depth + x], (owner, y * 2 + pu, px), same,
            )

    def finish_own():
        value = p0[r]
        for d in range(1, rows):
            i = order[d]
            arrived(r0.at[i], q_r0.at[i])
            value = value + r0[i]
        value = value.astype(jnp.bfloat16)
        cyc[y] = value
        for px in range(depth):
            mirror(0, y, px)
        rows_of = pl.ds(pl.multiple_of(y * width, width), width)
        turn[...] = jnp.dot(value, perm[rows_of, :], preferred_element_type=f32)

    def finish_other(h):
        value = p1[h, r]
        for d in range(1, rows):
            i = order[d]
            arrived(r1.at[h, i], q_r1.at[h, i])
            value = value + r1[h, i]
        value = value.astype(jnp.bfloat16)
        cyc[oy, :, pl.ds(h * lanes, lanes)] = value
        mirror(1, oy, h)
        rows_of = pl.ds(pl.multiple_of(oy * width + h * lanes, lanes), lanes)
        return turn[...] + jnp.dot(value, perm[rows_of, :], preferred_element_type=f32)

    other_product(0)
    finish_own()
    for h in range(1, depth):
        other_product(h)
        turn[...] = finish_other(h - 1)
    turned = finish_other(depth - 1)

    for to in range(cols):
        spread[to] = turned[:, to * lanes:(to + 1) * lanes].astype(jnp.bfloat16)
    place = pl.ds(pl.multiple_of(y * sub, sub), sub)
    for to in range(cols):
        send(spread.at[to], drecv.at[u, place, :], s_d.at[to], q_d.at[u, y], (r, to, x), c == to)

    for i in range(rows * depth):
        arrived(mrecv.at[i], q_m.at[i])
    for pu in range(2):
        for py in range(2):
            arrived(drecv.at[pu, pl.ds(py * sub, sub), :], q_d.at[pu, py])
        flipped = jnp.transpose(drecv[pu].astype(f32))
        for py in range(2):
            for g in range(groups):
                at = (py * groups + g) * strip
                a = (py * 2 + pu) * groups + g
                o_ref[a, 0] = mrecv[a].astype(f32) + flipped[at:at + strip, :]

    for copy, sent in pending:
        if sent is None:
            copy.wait_send()
        else:
            pl.when(sent)(copy.wait_send)


def planned(sizes, amplitudes, intermediate):
    rows, cols, depth, chunks = sizes
    band, kc = amplitudes.shape
    width = intermediate.shape[1]
    sub = band // (2 * depth)
    owners = rows * depth
    strip = width // owners
    lanes = band // depth
    bf16, f32 = jnp.bfloat16, jnp.float32
    dma = pltpu.SemaphoreType.DMA
    return pl.pallas_call(
        functools.partial(kernel, sizes),
        out_shape=jax.ShapeDtypeStruct((owners, 1, strip, lanes), f32),
        in_specs=[pl.BlockSpec(memory_space=pl.ANY)] * 2,
        out_specs=pl.BlockSpec(memory_space=pltpu.VMEM),
        scratch_shapes=[
            pltpu.VMEM((2, sub, kc), bf16),
            pltpu.VMEM((kc, width), bf16),
            pltpu.VMEM((sub, kc), bf16),
            pltpu.VMEM((rows, sub, kc), bf16),
            pltpu.VMEM((kc, width), bf16),
            pltpu.VMEM((rows, sub, width), f32),
            pltpu.VMEM((depth, rows, sub, lanes), f32),
            pltpu.VMEM((rows, sub, width), f32),
            pltpu.VMEM((depth, rows, sub, lanes), f32),
            pltpu.VMEM((sub, 2 * width), f32),
            pltpu.VMEM((2, sub, width), bf16),
            pltpu.VMEM((cols, sub, lanes), bf16),
            pltpu.VMEM((2 * width, 2 * width), bf16),
            pltpu.VMEM((2, 2 * sub, lanes), bf16),
            pltpu.VMEM((owners, strip, lanes), bf16),
            dma((4,)), dma((2, 4)), dma((2,)), dma((2, 4)), dma((depth, chunks)), dma((depth, chunks)),
            dma((rows,)), dma((rows,)), dma((depth, rows)), dma((2, depth, 2)), dma((cols,)),
            dma((2, 4)), dma((rows, 2)), dma((depth, chunks)), dma((depth, chunks)),
            dma((rows,)), dma((depth, rows)), dma((owners,)), dma((2, 2)),
        ],
        compiler_params=pltpu.CompilerParams(collective_id=0, has_side_effects=True),
    )(amplitudes, intermediate)


def solution(mesh):
    rows, cols, depth = (mesh.shape[name] for name in ("row", "col", "rep"))

    def local(amplitudes, intermediate):
        square = rows == cols == 2 * depth and depth == 2
        fits = amplitudes.shape[0] == intermediate.shape[1]
        if square and fits:
            return planned((rows, cols, depth, 4), amplitudes, intermediate)
        return general(amplitudes, intermediate)

    in_specs = (P("row", "col"), P("row", "col"))
    out_specs = P(None, "col", None, ("row", "rep"))
    return jax.shard_map(local, mesh=mesh, in_specs=in_specs, out_specs=out_specs, check_vma=False)
```
